32 devices in a mesh: grp: 4 (over y, core), rep: 8 (over z, x).
Axes of the slice: x: 2, y: 2, z: 4, core: 2. Of those that a mesh axis runs over, the one named last changes fastest.
Arguments:
- embeddings: bfloat16 [16384, 768], P(('grp', 'rep')), may hold values from -6 to 6
- cluster_ids: int32 [16384], P(('grp', 'rep')), may hold values from 0 to 12287, as said below
- owner_bounds: int32 [32], replicated, may hold values from 0 to 12287, as said below
Outputs:
- distance: float32 [16384], P(('grp', 'rep'))
- slot_index: int32 [16384], P(('grp', 'rep'))
- centroids: bfloat16 [32, 576, 768], P(('grp', 'rep'))
The draws below stay inside these ranges and needn't reach their ends.
Inputs may be any that keep to these rules, and one draw needn't show every extreme that they name: `cluster_ids`: in the rows of one device at most 48 rows belong to the clusters of one owner (owner o holds clusters owner_bounds[o] up to the next bound); in every draw some owner gets exactly 48 rows from every device. `owner_bounds`: owners are ordered grp first, then rep. The bounds rise from 0; each owner holds from 192 to 576 clusters, the last owner ending at 12288; some owner holds exactly 576.
All inputs are finite; a program needn't handle non-finite values.
Results may differ from the reference program's by a relative error of at most 0.004.
Values may be sent and summed in bfloat16 or wider, within the bound.
A program may use at most 128 MiB of HBM per device.

```python
import jax
import jax.numpy as jnp
from jax import lax

D = 768
ROWS_DEV = 512
CL_DEV = 384
OWNERS = 32
ROWS = 16384
SLOT = 48
OWN_MAX = 576


def owner_layout(key):
    half_count = OWNERS // 2
    spread = CL_DEV // 2
    base_key = jax.random.fold_in(key, 11)
    first_key, second_key, third_key, fourth_key = jax.random.split(base_key, 4)
    deltas = jax.random.randint(first_key, (half_count,), -spread, spread + 1)
    chosen = jax.random.randint(second_key, (), 0, half_count)
    deltas = jnp.where(jnp.arange(half_count) == chosen, spread, deltas)
    widths = jnp.concatenate([CL_DEV + deltas, CL_DEV - deltas]).astype(jnp.int32)
    widths = jax.random.permutation(third_key, widths)
    bounds = (jnp.cumsum(widths) - widths).astype(jnp.int32)
    busy_owner = jax.random.randint(fourth_key, (), 0, OWNERS).astype(jnp.int32)
    return (bounds, widths, busy_owner)


def draw_owner_bounds(key, part):
    return owner_layout(key)[0]


def draw_cluster_ids(key, part):
    bounds, widths, busy_owner = owner_layout(key)
    pool_size = (OWNERS - 1) * (SLOT - 1)

    def one_device(device_index):
        device_key = jax.random.fold_in(jax.random.fold_in(key, 23), device_index)
        first_key, second_key, third_key = jax.random.split(device_key, 3)
        owner_pool = jnp.arange(pool_size, dtype=jnp.int32) % (OWNERS - 1)
        chosen = jax.random.permutation(first_key, owner_pool)[:ROWS_DEV - SLOT]
        chosen = chosen + (chosen >= busy_owner).astype(jnp.int32)
        owner_of = jnp.concatenate([jnp.full((SLOT,), busy_owner, jnp.int32), chosen])
        offsets = jax.random.randint(second_key, (ROWS_DEV,), 0, 1 << 30) % widths[owner_of]
        identity = (bounds[owner_of] + offsets).astype(jnp.int32)
        return jax.random.permutation(third_key, identity)
    return jax.vmap(one_device)(jnp.arange(OWNERS)).reshape(-1)


def block_scale(rng, shape, shards, smallest, top_value):
    factor_of = 1.0
    for axis_at, shards_of in shards:
        heights = jax.random.uniform(jax.random.fold_in(jax.random.fold_in(rng, 6), axis_at), (shards_of,), jnp.float32, smallest / len(shards), top_value / len(shards))
        factor_of = factor_of * jnp.repeat(jnp.exp(heights), shape[axis_at] // shards_of).reshape((-1,) + (1,) * (len(shape) - 1 - axis_at))
    return factor_of


def noise(own_key, extent, deviation, bound, cuts=(), kind=jnp.bfloat16):
    array = deviation * jax.random.normal(own_key, extent, jnp.float32)
    if cuts:
        array = array * block_scale(own_key, extent, cuts, -0.22, 0.18)
    return jnp.clip(array, -bound, bound).astype(kind)


def setup_inputs(seed: int = 0) -> dict:
    key_list = jax.random.split(jax.random.key(seed), 4)
    embeddings = noise(key_list[0], (ROWS, D), 1.0, 6.0, ((0, 32),))
    cluster_ids = draw_cluster_ids(jax.random.fold_in(key_list[3], 71), 0)
    owner_bounds = draw_owner_bounds(jax.random.fold_in(key_list[3], 71), 0)
    return dict(embeddings=embeddings, cluster_ids=cluster_ids, owner_bounds=owner_bounds)


epsilon = 1e-06
norm_floor = 0.25

def normalize(block):
    values = block.astype(jnp.float32)
    return (values * lax.rsqrt(lax.optimization_barrier(jnp.sum(values * values, axis=1, keepdims=True)) + epsilon)).astype(jnp.bfloat16)

def reference(embeddings, cluster_ids, owner_bounds):
    clusters = CL_DEV * OWNERS
    row_count = embeddings.shape[0]
    unit_blocks = lax.map(normalize, embeddings.reshape(OWNERS, ROWS_DEV, D))
    id_blocks = cluster_ids.reshape(OWNERS, ROWS_DEV)

    def accumulate(block, carry):
        block_rows = lax.dynamic_index_in_dim(unit_blocks, block, 0, keepdims=False)
        block_ids = lax.dynamic_index_in_dim(id_blocks, block, 0, keepdims=False)
        return carry + jax.ops.segment_sum(block_rows.astype(jnp.float32), block_ids, num_segments=clusters)
    member_sums = lax.fori_loop(0, OWNERS, accumulate, jnp.zeros((clusters, D), jnp.float32))
    members = jax.ops.segment_sum(jnp.ones((row_count,), jnp.float32), cluster_ids, num_segments=clusters)
    centroid = member_sums / jnp.maximum(members, 1.0)[:, None]
    centroid_norm = jnp.sqrt(lax.optimization_barrier(jnp.sum(centroid * centroid, axis=1)))
    unit_centroid = (centroid / jnp.maximum(centroid_norm, norm_floor)[:, None]).astype(jnp.bfloat16)

    def measure(pair):
        block_rows, block_ids = pair
        picked = unit_centroid[block_ids]
        return 1.0 - lax.optimization_barrier(jnp.sum(block_rows.astype(jnp.float32) * picked.astype(jnp.float32), axis=1))
    distance = lax.map(measure, (unit_blocks, id_blocks)).reshape(-1)
    sorted_rows = jnp.argsort(cluster_ids, stable=True).astype(jnp.int32)
    sorted_place = jnp.zeros((row_count,), jnp.int32).at[sorted_rows].set(jnp.arange(row_count, dtype=jnp.int32))
    sorted_ids = cluster_ids[sorted_rows]
    slot_index = (sorted_place - jnp.searchsorted(sorted_ids, cluster_ids, side='left').astype(jnp.int32)).astype(jnp.int32)
    range_ends = jnp.concatenate([owner_bounds[1:], jnp.full((1,), clusters, jnp.int32)])
    wanted = owner_bounds[:, None] + jnp.arange(OWN_MAX, dtype=jnp.int32)[None, :]
    inside = wanted < range_ends[:, None]
    table = unit_centroid[jnp.minimum(wanted, clusters - 1)]
    centroids = jnp.where(inside[:, :, None], table, jnp.zeros_like(table)).astype(jnp.bfloat16)
    return (distance, slot_index, centroids)
```

```python
import functools

import jax
import jax.numpy as jnp
from jax import lax
from jax.experimental import pallas as pl
from jax.experimental.pallas import tpu as pltpu
from jax.sharding import PartitionSpec as P

CL_DEV = 384
LANES = 128

epsilon = 1e-06
norm_floor = 0.25
MESH = pl.DeviceIdType.MESH
F32 = jnp.float32
BF16 = jnp.bfloat16
EXACT = lax.Precision.HIGHEST
NT = (((1,), (1,)), ((), ()))


def iota(shape, dim):
    return lax.broadcasted_iota(jnp.int32, shape, dim)


def ones_at(mask, kind):
    return jnp.where(mask, 1.0, 0.0).astype(kind)


def digits_dot(table, place):
    high = jnp.floor(table * (1.0 / 32.0))
    low = table - 32.0 * high
    upper = jnp.dot(high.astype(BF16), place, preferred_element_type=F32)
    lower = jnp.dot(low.astype(BF16), place, preferred_element_type=F32)
    return 32.0 * upper + lower


def kernel(
    groups, replicas, slots,
    emb_ref, ids_ref, bounds_ref,
    cent_ref, dist_ref, rank_ref,
    unit, send_rows, got_rows, send_ids, got_ids, member, total, ret, got_ret, slot_mat,
    row_send, row_recv, id_send, id_recv, ret_send, ret_recv,
):
    my_group = lax.axis_index("grp")
    my_replica = lax.axis_index("rep")
    me = my_group * replicas + my_replica
    owners = groups * replicas
    rows, width = emb_ref.shape
    limit = cent_ref.shape[0]
    block = replicas * slots

    def peer(dg, dr):
        return lax.rem(my_group + dg, groups), lax.rem(my_replica + dr, replicas)

    def source(dg, dr):
        return (
            lax.rem(my_group + groups - dg, groups),
            lax.rem(my_replica + replicas - dr, replicas),
        )

    def every(dg, act):
        def one(dr, carry):
            act(dr)
            return carry

        lax.fori_loop(1 if dg == 0 else 0, replicas, one, 0)

    def copy(src, dst, ssem, rsem, pair, here, there):
        return pltpu.make_async_remote_copy(
            src_ref=src.at[there],
            dst_ref=dst.at[here],
            send_sem=ssem.at[there],
            recv_sem=rsem.at[here],
            device_id=pair,
            device_id_type=MESH,
        )

    def start(bufs, dg, dr):
        pair = peer(dg, dr)
        copy(*bufs, pair, me, pair[0] * replicas + pair[1]).start()

    def wait_send(bufs, dg, dr):
        pair = peer(dg, dr)
        copy(*bufs, pair, me, pair[0] * replicas + pair[1]).wait_send()

    def wait_recv(bufs, dg, dr):
        pair = source(dg, dr)
        there = pair[0] * replicas + pair[1]
        copy(*bufs, pair, there, there).wait_recv()

    row_bufs = (send_rows, got_rows, row_send, row_recv)
    id_bufs = (send_ids, got_ids, id_send, id_recv)
    ret_bufs = (ret, got_ret, ret_send, ret_recv)
    order = list(range(1, groups)) + [0]

    barrier = pltpu.get_barrier_semaphore()
    for dg in order:
        every(
            dg,
            lambda dr, dg=dg: pl.semaphore_signal(
                barrier, inc=1, device_id=peer(dg, dr), device_id_type=MESH
            ),
        )

    ids = ids_ref[...]
    edges = bounds_ref[...]
    reached = ones_at(edges <= ids, F32)
    owner = jnp.sum(reached, axis=0, keepdims=True).astype(jnp.int32) - 1
    owned = iota((owners, rows), 0) == owner
    owned_f = ones_at(owned, F32)
    first = jnp.sum(owned_f * edges.astype(F32), axis=0, keepdims=True)
    local = ids.astype(F32) - first
    earlier = ones_at(iota((rows, rows), 0) < iota((rows, rows), 1), BF16)
    prefix = jnp.dot(owned_f.astype(BF16), earlier, preferred_element_type=F32)
    rank = jnp.sum(owned_f * prefix, axis=0, keepdims=True).astype(jnp.int32)
    target = owner * slots + rank
    place = ones_at(iota((LANES, rows), 0) == rank, BF16)
    high = jnp.floor(local * (1.0 / 32.0))
    low = local - 32.0 * high
    upper = lax.dot_general((owned_f * high).astype(BF16), place, NT, preferred_element_type=F32)
    lower = lax.dot_general((owned_f * low).astype(BF16), place, NT, preferred_element_type=F32)
    filled = lax.dot_general(owned_f.astype(BF16), place, NT, preferred_element_type=F32)
    id_table = 32.0 * upper + lower + filled - 1.0
    for o in range(owners):
        send_ids[o] = jnp.broadcast_to(id_table[o : o + 1, :], (8, LANES))
    got_ids[me] = send_ids[me]

    values = emb_ref[...].astype(F32)
    unit[...] = (
        values * lax.rsqrt(jnp.sum(values * values, axis=1, keepdims=True) + epsilon)
    ).astype(BF16)

    pl.semaphore_wait(barrier, owners - 1)
    for dg in order:
        every(dg, lambda dr, dg=dg: start(id_bufs, dg, dr))
    for dg in order:
        tg = lax.rem(my_group + dg, groups)
        pick = ones_at(iota((block, rows), 0) + tg * block == target, BF16)
        packed = jnp.dot(pick, unit[...], preferred_element_type=F32).astype(BF16)
        send_rows[pl.ds(tg * replicas, replicas)] = packed.reshape(replicas, slots, width)
        every(dg, lambda dr, dg=dg: start(row_bufs, dg, dr))
    got_rows[me] = send_rows[me]

    for dg in order:
        every(dg, lambda dr, dg=dg: wait_recv(id_bufs, dg, dr))

    lane = iota((1, block), 1)
    quotient = jnp.zeros((1, block), jnp.int32)
    for s in range(1, replicas):
        quotient = quotient + jnp.where(lane >= s * slots, 1, 0)
    remainder = lane - quotient * slots
    spread = iota((LANES, block), 0) == remainder
    spread_b, spread_f = ones_at(spread, BF16), ones_at(spread, F32)
    from_source = ones_at(iota((replicas, block), 0) == quotient, F32)
    before = ones_at(iota((block, block), 0) < iota((block, block), 1), BF16)
    cluster = iota((limit, block), 0)

    seen = jnp.zeros((limit, 1), F32)
    for sg in range(groups):
        table = got_ids[sg * replicas : (sg + 1) * replicas, 0, :]
        flat = jnp.sum(from_source * digits_dot(table, spread_b), axis=0, keepdims=True)
        mask = ones_at(cluster == flat.astype(jnp.int32), F32)
        mask_b = mask.astype(BF16)
        member[sg] = mask_b
        ahead = jnp.dot(mask_b, before, preferred_element_type=F32) + seen
        slot = jnp.sum(mask * ahead, axis=0, keepdims=True)
        seen = seen + jnp.sum(mask, axis=1, keepdims=True)
        slot_mat[sg] = lax.dot_general(
            from_source * slot, spread_f, NT, precision=EXACT, preferred_element_type=F32
        )
    total[...] = jnp.zeros_like(total)
    for dg in order:
        sg = lax.rem(my_group + groups - dg, groups)
        every(dg, lambda dr, dg=dg: wait_recv(row_bufs, dg, dr))
        block_rows = got_rows[pl.ds(sg * replicas, replicas)].reshape(block, width)
        total[...] += jnp.dot(member[sg], block_rows, preferred_element_type=F32)

    centroid = total[...] / jnp.maximum(seen, 1.0)
    norm = jnp.sqrt(jnp.sum(centroid * centroid, axis=1, keepdims=True))
    cent_ref[...] = (centroid / jnp.maximum(norm, norm_floor)).astype(BF16)

    for dg in order:
        sg = lax.rem(my_group + groups - dg, groups)
        tg = lax.rem(my_group + groups - dg, groups)
        block_rows = got_rows[pl.ds(sg * replicas, replicas)].reshape(block, width)
        score = lax.dot_general(cent_ref[...], block_rows, NT, preferred_element_type=F32)
        near = jnp.sum(member[sg].astype(F32) * score, axis=0, keepdims=True)
        dist_mat = lax.dot_general(
            from_source * (1.0 - near), spread_f, NT, precision=EXACT, preferred_element_type=F32
        )
        rank_mat = slot_mat[sg]
        top = iota((8, LANES), 0) == 0
        for s in range(replicas):
            ret[tg * replicas + s] = jnp.where(top, dist_mat[s : s + 1, :], rank_mat[s : s + 1, :])
        back = (groups - dg) % groups
        every(back, lambda dr, back=back: start(ret_bufs, back, dr))
    got_ret[me] = ret[me]

    place_f = ones_at(iota((LANES, rows), 0) == rank, F32)
    for dg in order:
        every(dg, lambda dr, dg=dg: wait_recv(ret_bufs, dg, dr))
    dist_all = jnp.dot(got_ret[:, 0, :], place_f, precision=EXACT, preferred_element_type=F32)
    rank_all = jnp.dot(got_ret[:, 1, :], place_f, precision=EXACT, preferred_element_type=F32)
    dist_ref[...] = jnp.sum(owned_f * dist_all, axis=0, keepdims=True)
    rank_ref[...] = jnp.sum(owned_f * rank_all, axis=0, keepdims=True).astype(jnp.int32)
    for bufs in (id_bufs, row_bufs, ret_bufs):
        for dg in order:
            every(dg, lambda dr, dg=dg, bufs=bufs: wait_send(bufs, dg, dr))


def solution(mesh):
    groups, replicas = mesh.shape["grp"], mesh.shape["rep"]
    owners = groups * replicas

    def shards(embeddings, cluster_ids, owner_bounds):
        rows, width = embeddings.shape
        limit = CL_DEV + CL_DEV // 2
        slots = -(-(3 * rows // owners) // 16) * 16
        block = replicas * slots
        vmem = pl.BlockSpec(memory_space=pltpu.VMEM)
        small = pltpu.VMEM((owners, 8, LANES), F32)
        dma = pltpu.SemaphoreType.DMA((owners,))
        centroids, distance, rank = pl.pallas_call(
            functools.partial(kernel, groups, replicas, slots),
            out_shape=(
                jax.ShapeDtypeStruct((limit, width), BF16),
                jax.ShapeDtypeStruct((1, rows), F32),
                jax.ShapeDtypeStruct((1, rows), jnp.int32),
            ),
            in_specs=[vmem] * 3,
            out_specs=(vmem,) * 3,
            scratch_shapes=[
                pltpu.VMEM((rows, width), BF16),
                pltpu.VMEM((owners, slots, width), BF16),
                pltpu.VMEM((owners, slots, width), BF16),
                small,
                small,
                pltpu.VMEM((groups, limit, block), BF16),
                pltpu.VMEM((limit, width), F32),
                small,
                small,
                pltpu.VMEM((groups, replicas, LANES), F32),
                dma, dma, dma, dma, dma, dma,
            ],
            compiler_params=pltpu.CompilerParams(
                collective_id=0, has_side_effects=True, vmem_limit_bytes=56 * 1024 * 1024
            ),
        )(embeddings, cluster_ids.reshape(1, rows), owner_bounds.reshape(owners, 1))
        return distance.reshape(rows), rank.reshape(rows), centroids[None]

    placed = (P(("grp", "rep"), None), P(("grp", "rep")), P())
    return jax.shard_map(
        shards,
        mesh=mesh,
        in_specs=placed,
        out_specs=(P(("grp", "rep")), P(("grp", "rep")), P(("grp", "rep"), None, None)),
        check_vma=False,
    )
```

```python
import functools

import jax
import jax.numpy as jnp
from jax import lax
from jax.experimental import pallas as pl
from jax.experimental.pallas import tpu as pltpu
from jax.sharding import PartitionSpec as P

CL_DEV = 384
LANES = 128

epsilon = 1e-06
norm_floor = 0.25
MESH = pl.DeviceIdType.MESH
F32 = jnp.float32
BF16 = jnp.bfloat16
EXACT = lax.Precision.HIGHEST
NT = (((1,), (1,)), ((), ()))


def iota(shape, dim):
    return lax.broadcasted_iota(jnp.int32, shape, dim)


def ones_at(mask, kind):
    return jnp.where(mask, 1.0, 0.0).astype(kind)


def digits_dot(table, place):
    high = jnp.floor(table * (1.0 / 32.0))
    low = table - 32.0 * high
    upper = jnp.dot(high.astype(BF16), place, preferred_element_type=F32)
    lower = jnp.dot(low.astype(BF16), place, preferred_element_type=F32)
    return 32.0 * upper + lower


def kernel(
    groups, replicas, direct, extra,
    emb_ref, ids_ref, bounds_ref,
    cent_ref, dist_ref, rank_ref, over_ref,
    unit, send_rows, got_rows, send_ids, got_ids, member, total, ret, got_ret, slot_mat,
    row_send, row_recv, id_send, id_recv, ret_send, ret_recv,
    near_send, near_recv, far_send, far_recv,
):
    my_group = lax.axis_index("grp")
    my_replica = lax.axis_index("rep")
    me = my_group * replicas + my_replica
    owners = groups * replicas
    rows, width = emb_ref.shape
    limit = cent_ref.shape[0]
    slots = direct + extra
    block = replicas * slots
    sent = replicas * direct

    def peer(dg, dr):
        return lax.rem(my_group + dg, groups), lax.rem(my_replica + dr, replicas)

    def source(dg, dr):
        return (
            lax.rem(my_group + groups - dg, groups),
            lax.rem(my_replica + replicas - dr, replicas),
        )

    def every(dg, act):
        def one(dr, carry):
            act(dr)
            return carry

        lax.fori_loop(1 if dg == 0 else 0, replicas, one, 0)

    def copy(src, dst, ssem, rsem, pair, here, there):
        return pltpu.make_async_remote_copy(
            src_ref=src.at[there],
            dst_ref=dst.at[here, pl.ds(0, direct)] if dst is got_rows else dst.at[here],
            send_sem=ssem.at[there],
            recv_sem=rsem.at[here],
            device_id=pair,
            device_id_type=MESH,
        )

    def start(bufs, dg, dr):
        pair = peer(dg, dr)
        copy(*bufs, pair, me, pair[0] * replicas + pair[1]).start()

    def wait_send(bufs, dg, dr):
        pair = peer(dg, dr)
        copy(*bufs, pair, me, pair[0] * replicas + pair[1]).wait_send()

    def wait_recv(bufs, dg, dr):
        pair = source(dg, dr)
        there = pair[0] * replicas + pair[1]
        copy(*bufs, pair, there, there).wait_recv()

    row_bufs = (send_rows, got_rows, row_send, row_recv)
    id_bufs = (send_ids, got_ids, id_send, id_recv)
    ret_bufs = (ret, got_ret, ret_send, ret_recv)
    order = list(range(1, groups)) + [0]

    barrier = pltpu.get_barrier_semaphore()
    for dg in order:
        every(
            dg,
            lambda dr, dg=dg: pl.semaphore_signal(
                barrier, inc=1, device_id=peer(dg, dr), device_id_type=MESH
            ),
        )

    ids = ids_ref[...]
    edges = bounds_ref[...]
    reached = ones_at(edges <= ids, F32)
    owner = jnp.sum(reached, axis=0, keepdims=True).astype(jnp.int32) - 1
    owned = iota((owners, rows), 0) == owner
    owned_f = ones_at(owned, F32)
    first = jnp.sum(owned_f * edges.astype(F32), axis=0, keepdims=True)
    local = ids.astype(F32) - first
    earlier = ones_at(iota((rows, rows), 0) < iota((rows, rows), 1), BF16)
    prefix = jnp.dot(owned_f.astype(BF16), earlier, preferred_element_type=F32)
    rank = jnp.sum(owned_f * prefix, axis=0, keepdims=True).astype(jnp.int32)
    target = jnp.where(rank < direct, owner * direct + rank, -1)
    spot = rank
    if extra:
        late = ones_at(rank >= direct, F32)
        queue = jnp.dot(
            jnp.broadcast_to(late, (8, rows)).astype(BF16), earlier, preferred_element_type=F32
        )[0:1, :].astype(jnp.int32)
        spot = jnp.where(rank < direct, rank, direct + queue)
    place = ones_at(iota((LANES, rows), 0) == spot, BF16)

    values = emb_ref[...].astype(F32)
    unit[...] = (
        values * lax.rsqrt(jnp.sum(values * values, axis=1, keepdims=True) + epsilon)
    ).astype(BF16)

    def pack(dg):
        tg = lax.rem(my_group + dg, groups)
        pick = ones_at(iota((sent, rows), 0) + tg * sent == target, BF16)
        packed = jnp.dot(pick, unit[...], preferred_element_type=F32).astype(BF16)
        send_rows[pl.ds(tg * replicas, replicas)] = packed.reshape(replicas, direct, width)

    def near_copy(pair, owner_at, dr):
        ref = got_rows.at[owner_at, pl.ds(direct, extra)]
        return pltpu.make_async_remote_copy(
            src_ref=ref, dst_ref=ref, send_sem=near_send.at[dr], recv_sem=near_recv.at[dr],
            device_id=pair, device_id_type=MESH,
        )

    def far_copy(group_at, to_group, dg):
        ref = got_rows.at[pl.ds(group_at * replicas, replicas), pl.ds(direct, extra)]
        return pltpu.make_async_remote_copy(
            src_ref=ref, dst_ref=ref, send_sem=far_send.at[dg], recv_sem=far_recv.at[dg],
            device_id=(to_group, my_replica), device_id_type=MESH,
        )

    if extra:
        pick = ones_at(iota((extra, rows), 0) + direct == spot, BF16)
        got_rows[me, direct:slots] = jnp.dot(
            pick, unit[...], preferred_element_type=F32
        ).astype(BF16)
    pack(order[0])
    pl.semaphore_wait(barrier, owners - 1)
    if extra:
        every(0, lambda dr: near_copy(peer(0, dr), me, dr).start())
    every(order[0], lambda dr: start(row_bufs, order[0], dr))

    high = jnp.floor(local * (1.0 / 32.0))
    low = local - 32.0 * high
    owned_d = jnp.where(rank < direct, owned_f, 0.0)
    upper = lax.dot_general((owned_d * high).astype(BF16), place, NT, preferred_element_type=F32)
    lower = lax.dot_general((owned_d * low).astype(BF16), place, NT, preferred_element_type=F32)
    filled = lax.dot_general(owned_d.astype(BF16), place, NT, preferred_element_type=F32)
    id_table = 32.0 * upper + lower + filled - 1.0
    count = jnp.zeros((1, 1), F32)
    if extra:
        named = jnp.broadcast_to(late * (ids.astype(F32) + 1.0), (8, rows))
        others = lax.dot_general(
            named, place.astype(F32), NT, precision=EXACT, preferred_element_type=F32
        )
        id_table = id_table + others[0:1, :]
        count = jnp.sum(late, axis=1, keepdims=True)
    top = iota((8, LANES), 0) == 0
    for o in range(owners):
        send_ids[o] = jnp.where(top, id_table[o : o + 1, :], count)
    got_ids[me] = send_ids[me]

    for dg in order:
        every(dg, lambda dr, dg=dg: start(id_bufs, dg, dr))
    for dg in order[1:]:
        pack(dg)
        every(dg, lambda dr, dg=dg: start(row_bufs, dg, dr))
    got_rows[me, 0:direct] = send_rows[me]
    if extra:
        def near_wait(dr):
            pair = source(0, dr)
            near_copy(pair, pair[0] * replicas + pair[1], dr).wait_recv()

        every(0, near_wait)
        for dg in order[:-1]:
            far_copy(my_group, lax.rem(my_group + dg, groups), dg).start()

    for dg in order:
        every(dg, lambda dr, dg=dg: wait_recv(id_bufs, dg, dr))
    worst = jnp.max(got_ids[:, 1, :], axis=0, keepdims=True)
    over_ref[...] = jnp.where(worst > extra, 1, 0)
    begin = jnp.sum(
        jnp.where(iota((owners, 1), 0) == me, edges, 0), axis=0, keepdims=True
    ).astype(F32)
    ending = jnp.sum(
        jnp.where(iota((owners, 1), 0) == me + 1, edges, 0), axis=0, keepdims=True
    ).astype(F32) + jnp.where(me == owners - 1, float(CL_DEV * owners), 0.0)

    lane = iota((1, block), 1)
    quotient = jnp.zeros((1, block), jnp.int32)
    for s in range(1, replicas):
        quotient = quotient + jnp.where(lane >= s * slots, 1, 0)
    remainder = lane - quotient * slots
    spread = iota((LANES, block), 0) == remainder
    spread_b, spread_f = ones_at(spread, BF16), ones_at(spread, F32)
    from_source = ones_at(iota((replicas, block), 0) == quotient, F32)
    before = ones_at(iota((block, block), 0) < iota((block, block), 1), BF16)
    cluster = iota((limit, block), 0)

    seen = jnp.zeros((limit, 1), F32)
    for sg in range(groups):
        table = got_ids[sg * replicas : (sg + 1) * replicas, 0, :]
        if extra:
            mine = jnp.where((table >= begin) & (table < ending), table - begin, -1.0)
            table = jnp.where(iota((replicas, LANES), 1) < direct, table, mine)
        flat = jnp.sum(from_source * digits_dot(table, spread_b), axis=0, keepdims=True)
        mask = ones_at(cluster == flat.astype(jnp.int32), F32)
        mask_b = mask.astype(BF16)
        member[sg] = mask_b
        ahead = jnp.dot(mask_b, before, preferred_element_type=F32) + seen
        slot = jnp.sum(mask * ahead, axis=0, keepdims=True)
        seen = seen + jnp.sum(mask, axis=1, keepdims=True)
        slot_mat[sg] = lax.dot_general(
            from_source * slot, spread_f, NT, precision=EXACT, preferred_element_type=F32
        )
    total[...] = jnp.zeros_like(total)
    for dg in order:
        sg = lax.rem(my_group + groups - dg, groups)
        every(dg, lambda dr, dg=dg: wait_recv(row_bufs, dg, dr))
        if extra and dg:
            far_copy(sg, sg, dg).wait_recv()
        block_rows = got_rows[pl.ds(sg * replicas, replicas)].reshape(block, width)
        total[...] += jnp.dot(member[sg], block_rows, preferred_element_type=F32)

    centroid = total[...] / jnp.maximum(seen, 1.0)
    norm = jnp.sqrt(jnp.sum(centroid * centroid, axis=1, keepdims=True))
    cent_ref[...] = (centroid / jnp.maximum(norm, norm_floor)).astype(BF16)

    for dg in order:
        sg = lax.rem(my_group + groups - dg, groups)
        tg = lax.rem(my_group + groups - dg, groups)
        block_rows = got_rows[pl.ds(sg * replicas, replicas)].reshape(block, width)
        score = lax.dot_general(cent_ref[...], block_rows, NT, preferred_element_type=F32)
        near = jnp.sum(member[sg].astype(F32) * score, axis=0, keepdims=True)
        dist_mat = lax.dot_general(
            from_source * (1.0 - near), spread_f, NT, precision=EXACT, preferred_element_type=F32
        )
        rank_mat = slot_mat[sg]
        for s in range(replicas):
            ret[tg * replicas + s] = jnp.where(top, dist_mat[s : s + 1, :], rank_mat[s : s + 1, :])
        back = (groups - dg) % groups
        every(back, lambda dr, back=back: start(ret_bufs, back, dr))
    got_ret[me] = ret[me]

    place_f = ones_at(iota((LANES, rows), 0) == spot, F32)
    for dg in order:
        every(dg, lambda dr, dg=dg: wait_recv(ret_bufs, dg, dr))
    dist_all = jnp.dot(got_ret[:, 0, :], place_f, precision=EXACT, preferred_element_type=F32)
    rank_all = jnp.dot(got_ret[:, 1, :], place_f, precision=EXACT, preferred_element_type=F32)
    dist_ref[...] = jnp.sum(owned_f * dist_all, axis=0, keepdims=True)
    rank_ref[...] = jnp.sum(owned_f * rank_all, axis=0, keepdims=True).astype(jnp.int32)
    for bufs in (id_bufs, row_bufs, ret_bufs):
        for dg in order:
            every(dg, lambda dr, dg=dg, bufs=bufs: wait_send(bufs, dg, dr))
    if extra:
        every(0, lambda dr: near_copy(peer(0, dr), me, dr).wait_send())
        for dg in order[:-1]:
            far_copy(my_group, lax.rem(my_group + dg, groups), dg).wait_send()


def solution(mesh):
    groups, replicas = mesh.shape["grp"], mesh.shape["rep"]
    owners = groups * replicas

    def shards(embeddings, cluster_ids, owner_bounds):
        rows, width = embeddings.shape
        limit = CL_DEV + CL_DEV // 2
        most = -(-(3 * rows // owners) // 16) * 16
        direct = -(-2 * most // 48) * 16
        vmem = pl.BlockSpec(memory_space=pltpu.VMEM)
        small = pltpu.VMEM((owners, 8, LANES), F32)
        each = pltpu.SemaphoreType.DMA((owners,))
        near = pltpu.SemaphoreType.DMA((replicas,))
        far = pltpu.SemaphoreType.DMA((groups,))
        ids_row, edges = cluster_ids.reshape(1, rows), owner_bounds.reshape(owners, 1)

        def run(direct, extra, number):
            slots = direct + extra
            return pl.pallas_call(
                functools.partial(kernel, groups, replicas, direct, extra),
                out_shape=(
                    jax.ShapeDtypeStruct((limit, width), BF16),
                    jax.ShapeDtypeStruct((1, rows), F32),
                    jax.ShapeDtypeStruct((1, rows), jnp.int32),
                    jax.ShapeDtypeStruct((1, LANES), jnp.int32),
                ),
                in_specs=[vmem] * 3,
                out_specs=(vmem,) * 4,
                scratch_shapes=[
                    pltpu.VMEM((rows, width), BF16),
                    pltpu.VMEM((owners, direct, width), BF16),
                    pltpu.VMEM((owners, slots, width), BF16),
                    small,
                    small,
                    pltpu.VMEM((groups, limit, replicas * slots), BF16),
                    pltpu.VMEM((limit, width), F32),
                    small,
                    small,
                    pltpu.VMEM((groups, replicas, LANES), F32),
                    each, each, each, each, each, each, near, near, far, far,
                ],
                compiler_params=pltpu.CompilerParams(
                    collective_id=number,
                    has_side_effects=True,
                    vmem_limit_bytes=48 * 1024 * 1024,
                ),
            )(embeddings, ids_row, edges)

        if direct >= most:
            centroids, distance, rank, _ = run(most, 0, 0)
        else:
            first = run(direct, most - direct, 0)
            centroids, distance, rank = lax.cond(
                first[3][0, 0] > 0, lambda: run(most, 0, 1)[:3], lambda: first[:3]
            )
        return distance.reshape(rows), rank.reshape(rows), centroids[None]

    placed = (P(("grp", "rep"), None), P(("grp", "rep")), P())
    return jax.shard_map(
        shards,
        mesh=mesh,
        in_specs=placed,
        out_specs=(P(("grp", "rep")), P(("grp", "rep")), P(("grp", "rep"), None, None)),
        check_vma=False,
    )
```
